32 devices in a mesh: dp: 1 (over z), cy: 4 (over y), cx: 4 (over x), core: 2 (over core).
Axes of the slice: x: 4, y: 4, z: 1, core: 2. Of those that a mesh axis runs over, the one named last changes fastest.
The devices are a block of a 4x4x8 slice.
Arguments:
- x_in: bfloat16 [1, 3072, 2048], P('dp', ('cy', 'cx', 'core'))
- w_qkv: bfloat16 [2048, 32, 128], replicated
- w_out: bfloat16 [16, 128, 2048], replicated
Outputs:
- output: bfloat16 [1, 3072, 2048], P('dp', ('cy', 'cx', 'core'))
All inputs are finite; a program needn't handle non-finite values.
Results may differ from the reference program's by a relative error of at most 0.00801081.
Values are sent between devices in bfloat16 or wider.
A program may use at most 768 MiB of HBM per device.

```python
import math
import jax
import jax.numpy as jnp
from jax import lax

TOKENS_DEV = 96
GROUP_DEVICES = 32
HEADS = 16
KV_HEADS = 8
HEAD_DIM = 128

TOKENS = TOKENS_DEV * GROUP_DEVICES
WIDTH = HEADS * HEAD_DIM
GROUP_SIZE = HEADS // KV_HEADS
QUERY_GAIN = 2.0
OUT_GAIN = math.sqrt(TOKENS) * math.exp(-0.5 * QUERY_GAIN ** 2)


def setup_inputs(seed: int = 0, part: int = 0) -> dict:
    root_key = jax.random.key(seed)
    key_act = jax.random.fold_in(jax.random.fold_in(root_key, 1), part)
    key_qkv = jax.random.fold_in(root_key, 2)
    key_out = jax.random.fold_in(root_key, 3)
    act_rows = jax.random.normal(key_act, (1, TOKENS, WIDTH), jnp.float32)
    head_gain = jnp.concatenate([jnp.full((HEADS,), QUERY_GAIN, jnp.float32), jnp.ones((2 * KV_HEADS,), jnp.float32)])
    w_qkv = jax.random.normal(key_qkv, (WIDTH, HEADS + 2 * KV_HEADS, HEAD_DIM), jnp.float32) * (WIDTH ** -0.5) * head_gain[None, :, None]
    w_out = jax.random.normal(key_out, (HEADS, HEAD_DIM, WIDTH), jnp.float32) * (OUT_GAIN * WIDTH ** -0.5)
    return {"x_in": act_rows.astype(jnp.bfloat16), "w_qkv": w_qkv.astype(jnp.bfloat16), "w_out": w_out.astype(jnp.bfloat16)}


def reference(x_in, w_qkv, w_out):
    qkv_rows = jnp.dot(x_in[0], w_qkv.reshape(WIDTH, -1), preferred_element_type=jnp.float32)
    qkv_rows = qkv_rows.astype(jnp.bfloat16).reshape(TOKENS, HEADS + 2 * KV_HEADS, HEAD_DIM)
    queries = qkv_rows[:, :HEADS].reshape(GROUP_DEVICES, TOKENS_DEV, KV_HEADS, GROUP_SIZE, HEAD_DIM)
    queries = jnp.transpose(queries, (2, 0, 1, 3, 4))
    key_heads = jnp.transpose(qkv_rows[:, HEADS:HEADS + KV_HEADS], (1, 0, 2))
    value_heads = jnp.transpose(qkv_rows[:, HEADS + KV_HEADS:], (1, 0, 2))
    logit_scale = HEAD_DIM ** -0.5

    def head_attend(operands):
        q_head, k_head, v_head = operands
        k_wide = k_head.astype(jnp.float32)
        v_wide = v_head.astype(jnp.float32)

        def tile_attend(q_tile):
            scores = jnp.einsum("qgd,sd->gqs", q_tile.astype(jnp.float32), k_wide) * logit_scale
            weights = jax.nn.softmax(scores, axis=-1)
            return jnp.einsum("gqs,sd->qgd", weights, v_wide)

        return lax.map(tile_attend, q_head)

    attn_out = lax.map(head_attend, (queries, key_heads, value_heads))
    attn_out = jnp.transpose(attn_out, (1, 2, 0, 3, 4)).reshape(TOKENS, WIDTH).astype(jnp.bfloat16)
    y_rows = jnp.dot(attn_out, w_out.reshape(WIDTH, WIDTH), preferred_element_type=jnp.float32)
    return y_rows.astype(jnp.bfloat16)[None]
```

```python
import functools
import math

import jax
import jax.numpy as jnp
from jax import lax
from jax.experimental import pallas as pl
from jax.experimental.pallas import tpu as pltpu
from jax.sharding import PartitionSpec as P

MESH = pl.DeviceIdType.MESH
F32 = jnp.float32
BF16 = jnp.bfloat16


def kernel(n, x_hbm, w_hbm, wo_hbm, y_ref,
           xbuf, xil, wstage, wn, wo, kvout, qout, kvb, qb, acc, mrun, lrun, osend, orecv,
           sem_x, sem_w, sem_wo, sx_send, sx_recv, s_kv1, r_kv1, s_q1, r_q1,
           s_kv2, r_kv2, s_kv3, r_kv3, s_o, r_o):
    dp = lax.axis_index("dp")
    cy = lax.axis_index("cy")
    cx = lax.axis_index("cx")
    c = lax.axis_index("core")
    a = cx * (1 - c) + cy * c
    b = cy * (1 - c) + cx * c
    tok = xbuf.shape[1]
    dim = kvb.shape[-1]
    chip = 2 * tok
    width = xbuf.shape[2]
    half = 4 // n

    def dev(da, db, core):
        ra = lax.rem(a + da + n, n)
        rb = lax.rem(b + db + n, n)
        return (dp, rb * (1 - c) + ra * c, ra * (1 - c) + rb * c, core)

    def remote(src, dst, ssem, rsem, device):
        return pltpu.make_async_remote_copy(
            src_ref=src, dst_ref=dst, send_sem=ssem, recv_sem=rsem, device_id=device, device_id_type=MESH)

    x_cp = pltpu.make_async_copy(x_hbm.at[0], xbuf.at[c], sem_x)
    x_cp.start()
    npair = w_hbm.shape[1]
    nq, nkv = npair // 2, npair // 4
    own = nq // 2
    pairs = []
    for i in range(own // 2):
        pairs += [nq + (own // 2) * c + i, nq + nkv + (own // 2) * c + i]
    for i in range(own):
        pairs.append(own * c + i)
    w_cps = [pltpu.make_async_copy(w_hbm.at[:, p], wstage.at[i], sem_w.at[i]) for i, p in enumerate(pairs)]
    for cp in w_cps:
        cp.start()

    barrier = pltpu.get_barrier_semaphore()
    peers = [dev(0, 0, 1 - c)]
    for d in range(1, n):
        for core in (c, 1 - c):
            peers += [dev(d, 0, core), dev(0, d, core)]
    for p in peers:
        pl.semaphore_signal(barrier, inc=1, device_id=p, device_id_type=MESH)

    def expand(core):
        er = lax.broadcasted_iota(jnp.int32, (dim, 4 * dim), 0)
        ec = lax.broadcasted_iota(jnp.int32, (dim, 4 * dim), 1)
        sel = jnp.where(ec < 2 * dim, 2 * er, 2 * dim + 2 * er + 1)
        e = jnp.where(ec == sel, 1.0, 0.0).astype(BF16)
        nb = width // dim
        r0 = pl.multiple_of(core * tok, tok)
        r1 = pl.multiple_of(chip + core * tok, tok)
        step = 4
        for j0 in range(0, nb, step):
            xs = jnp.concatenate([xbuf[core, :, (j0 + j) * dim:(j0 + j + 1) * dim] for j in range(step)], axis=0)
            r = jnp.dot(xs, e, preferred_element_type=F32).astype(BF16)
            for j in range(step):
                cols = slice((j0 + j) * 2 * dim, (j0 + j + 1) * 2 * dim)
                xil[pl.ds(r0, tok), cols] = r[j * tok:(j + 1) * tok, :2 * dim]
                xil[pl.ds(r1, tok), cols] = r[j * tok:(j + 1) * tok, 2 * dim:]

    x_cp.wait()
    pl.semaphore_wait(barrier, len(peers))
    x_rc = remote(xbuf.at[c], xbuf.at[c], sx_send, sx_recv, dev(0, 0, 1 - c))
    x_rc.start()
    expand(c)

    rows = 2 * w_hbm.shape[0]
    blk = 256
    for i in range(len(pairs)):
        w_cps[i].wait()

        def relay(t, _, i=i):
            k0 = pl.multiple_of(t * (blk // 2), blk // 2)
            r0 = pl.multiple_of(t * blk, blk)
            wn[i // 2, pl.ds(r0, blk), (i % 2) * dim:(i % 2 + 1) * dim] = \
                wstage[i, pl.ds(k0, blk // 2)].reshape(blk, dim)
            return 0

        lax.fori_loop(0, rows // blk, relay, 0)
    wo_cps = []
    for g in range(wo.shape[0]):
        cp = pltpu.make_async_copy(wo_hbm.at[g], wo.at[g], sem_wo.at[g])
        cp.start()
        wo_cps.append(cp)

    x_rc.wait_recv()
    expand(1 - c)

    for i in range(own // 2):
        r = jnp.dot(xil[...], wn[i], preferred_element_type=F32).astype(BF16)
        for e in range(2):
            for kv in range(2):
                kvout[2 * i + e, kv] = r[e * chip:(e + 1) * chip, kv * dim:(kv + 1) * dim]
    mine = pl.ds(pl.multiple_of(a * chip, chip), chip)
    sends = []
    for k, d in enumerate((2, 1, 3)):
        cp = remote(kvout.at[lax.rem(a + d, n)], kvb.at[0, :, mine], s_kv1.at[k], r_kv1.at[a], dev(d, 0, c))
        cp.start()
        sends.append(cp)

    def forward(src, piece):
        where = pl.ds(pl.multiple_of(piece * chip, chip), chip)
        for k, d in enumerate((1, -1)):
            cp = remote(src, kvb.at[1 + k, :, where], s_kv2.at[k, piece], r_kv2.at[k, piece], dev(0, d, c))
            cp.start()

    forward(kvout.at[a], a)
    for i in range(own // 2):
        r = jnp.dot(xil[...], wn[own // 2 + i], preferred_element_type=F32).astype(BF16)
        for e in range(2):
            for h in range(2):
                qout[2 * i + e, h] = r[h * chip:(h + 1) * chip, e * dim:(e + 1) * dim]
    for k, d in enumerate((2, 1, 3)):
        cp = remote(qout.at[lax.rem(a + d, n)], qb.at[:, mine], s_q1.at[k], r_q1.at[a], dev(d, 0, c))
        cp.start()
        sends.append(cp)
    kvb[0, :, mine] = kvout[a]
    qb[:, mine] = qout[a]

    def recv(dst, sem):
        remote(dst, dst, s_kv1.at[0], sem, dev(1, 0, c)).wait_recv()

    for d in (1, 3, 2):
        piece = lax.rem(a + d, n)
        where = pl.ds(pl.multiple_of(piece * chip, chip), chip)
        recv(kvb.at[0, :, where], r_kv1.at[piece])
        forward(kvb.at[0, :, where], piece)
    for d in (1, 3, 2):
        piece = lax.rem(a + d, n)
        where = pl.ds(pl.multiple_of(piece * chip, chip), chip)
        recv(qb.at[:, where], r_q1.at[piece])

    scale = dim ** -0.5 * math.log2(math.e)

    def attend(block, t, first, last):
        rows = pl.ds(pl.multiple_of(t * chip, chip), chip)
        q = qb[:, rows].reshape(2 * chip, dim)
        keys = kvb.shape[2]
        s = lax.dot_general(q, kvb[block, 0], (((1,), (1,)), ((), ())), preferred_element_type=F32)
        m_new = jnp.max(s, axis=1, keepdims=True)
        if not first:
            m_old = mrun[t][:, :1]
            m_new = jnp.maximum(m_new, m_old)
            alpha = jnp.exp2((m_old - m_new) * scale)
        p = jnp.exp2((s - m_new) * scale)
        l = p[:, :dim]
        for j in range(1, keys // dim):
            l = l + p[:, j * dim:(j + 1) * dim]
        o = jnp.dot(p.astype(BF16), kvb[block, 1], preferred_element_type=F32)
        if not first:
            l = lrun[t] * alpha + l
            o = acc[t] * alpha + o
        if last:
            o = (o / jnp.sum(l, axis=1, keepdims=True)).astype(BF16)
            osend[t] = o.reshape(2, chip, dim)
        else:
            mrun[t] = jnp.broadcast_to(m_new, (2 * chip, dim))
            lrun[t] = l
            acc[t] = o

    def attend_all(block, first):
        for t in range(n):
            attend(block, t, first, False)

    attend_all(0, True)

    def spot(p):
        return pl.ds(p * chip, chip)

    h = n // 2
    for p in range(h):
        recv(kvb.at[1, :, spot(p)], r_kv2.at[0, p])
        remote(kvb.at[1, :, spot(p)], kvb.at[3, :, spot(p)], s_kv3.at[p], r_kv3.at[p], dev(0, 1, c)).start()
    for p in range(h, n):
        recv(kvb.at[2, :, spot(p)], r_kv2.at[1, p])
        remote(kvb.at[2, :, spot(p)], kvb.at[3, :, spot(p)], s_kv3.at[p], r_kv3.at[p], dev(0, -1, c)).start()
    for p in range(h, n):
        recv(kvb.at[1, :, spot(p)], r_kv2.at[0, p])
    attend_all(1, False)
    for p in range(h):
        recv(kvb.at[2, :, spot(p)], r_kv2.at[1, p])
    attend_all(2, False)
    for p in range(n):
        recv(kvb.at[3, :, spot(p)], r_kv3.at[p])

    head = own * c + a
    for k, d in enumerate((2, 1, 3, 0)):
        t = lax.rem(a + d, n)
        attend(3, t, False, True)
        for e in range(2):
            core = c if e == 0 else 1 - c
            part = pl.ds(pl.multiple_of(core * tok, tok), tok)
            if d == 0 and e == 0:
                orecv[head] = osend[t, :, part]
            else:
                cp = remote(osend.at[t, :, part], orecv.at[head], s_o.at[k, e], r_o.at[head], dev(d, 0, core))
                cp.start()
                sends.append(cp)

    order = [(0, 0), (0, 1), (1, 0), (1, 1), (3, 0), (3, 1), (2, 0), (2, 1)]
    for cp in wo_cps:
        cp.wait()
    for k, (d, e) in enumerate(order):
        if e == 0:
            g = own * c + lax.rem(a + d, n)
        else:
            g = own * (1 - c) + lax.rem(b + d, n)
        if k > 0:
            recv(orecv.at[g], r_o.at[g])
        o = jnp.concatenate([orecv[g, 0], orecv[g, 1]], axis=1)
        r = jnp.dot(o, wo[g], preferred_element_type=F32)
        if k == 0:
            yacc = r
        else:
            yacc = yacc + r
    y_ref[0] = yacc.astype(BF16)

    x_rc.wait_send()
    for cp in sends:
        cp.wait_send()
    for p in range(n):
        for k, d in enumerate((1, -1)):
            remote(kvb.at[0, :, spot(p)], kvb.at[1 + k, :, spot(p)], s_kv2.at[k, p], r_kv2.at[k, p],
                   dev(0, d, c)).wait_send()
        remote(kvb.at[1, :, spot(p)], kvb.at[3, :, spot(p)], s_kv3.at[p], r_kv3.at[p], dev(0, 1, c)).wait_send()


def solution(mesh):
    n = mesh.shape["cx"]
    assert mesh.shape["cy"] == n and n == 4 and mesh.shape["core"] == 2
    seq_spec = P("dp", ("cy", "cx", "core"))

    def local_layer(x_loc, w_qkv, w_out):
        _, tok, width = x_loc.shape
        heads, dim, out_width = w_out.shape
        all_heads = w_qkv.shape[1]
        kv = (all_heads - heads) // 2
        assert kv == 2 * n and heads == 2 * kv
        chip = 2 * tok
        keys = n * chip
        w_pairs = w_qkv.reshape(width, all_heads // 2, 2, dim)
        wo_pairs = w_out.reshape(kv, 2 * dim, out_width)
        dma = pltpu.SemaphoreType.DMA
        return pl.pallas_call(
            functools.partial(kernel, n),
            out_shape=jax.ShapeDtypeStruct(x_loc.shape, BF16),
            in_specs=[pl.BlockSpec(memory_space=pl.ANY)] * 3,
            out_specs=pl.BlockSpec(memory_space=pltpu.VMEM),
            scratch_shapes=[
                pltpu.VMEM((2, tok, width), BF16),
                pltpu.VMEM((2 * chip, 2 * width), BF16),
                pltpu.VMEM((kv, width, 2, dim), BF16),
                pltpu.VMEM((kv // 2, 2 * width, 2 * dim), BF16),
                pltpu.VMEM((kv, 2 * dim, out_width), BF16),
                pltpu.VMEM((n, 2, chip, dim), BF16),
                pltpu.VMEM((n, 2, chip, dim), BF16),
                pltpu.VMEM((4, 2, keys, dim), BF16),
                pltpu.VMEM((2, keys, dim), BF16),
                pltpu.VMEM((n, 2 * chip, dim), F32),
                pltpu.VMEM((n, 2 * chip, dim), F32),
                pltpu.VMEM((n, 2 * chip, dim), F32),
                pltpu.VMEM((n, 2, chip, dim), BF16),
                pltpu.VMEM((kv, 2, tok, dim), BF16),
                dma, dma((kv,)), dma((kv,)),
                dma, dma,
                dma((3,)), dma((n,)), dma((3,)), dma((n,)),
                dma((2, n)), dma((2, n)), dma((n,)), dma((n,)),
                dma((n, 2)), dma((kv,)),
            ],
            compiler_params=pltpu.CompilerParams(
                collective_id=0, has_side_effects=True, vmem_limit_bytes=60 * 1024 * 1024),
        )(x_loc, w_pairs, wo_pairs)

    return jax.shard_map(local_layer, mesh=mesh, in_specs=(seq_spec, P(), P()), out_specs=seq_spec, check_vma=False)
```

```python
import functools
import math

import jax
import jax.numpy as jnp
from jax import lax
from jax.experimental import pallas as pl
from jax.experimental.pallas import tpu as pltpu
from jax.sharding import PartitionSpec as P

MESH = pl.DeviceIdType.MESH
F32 = jnp.float32
BF16 = jnp.bfloat16


def kernel(n, x_hbm, w_hbm, wo_hbm, y_ref,
           xbuf, xil, wstage, wo, kvout, qout, kvb, qb, acc, mrun, lrun, osend, orecv,
           sem_x, sem_w, sem_wo, sx_send, sx_recv, s_kv1, r_kv1, s_q1, r_q1,
           s_kv2, r_kv2, s_kv3, r_kv3, s_o, r_o):
    dp = lax.axis_index("dp")
    cy = lax.axis_index("cy")
    cx = lax.axis_index("cx")
    c = lax.axis_index("core")
    a = cx * (1 - c) + cy * c
    b = cy * (1 - c) + cx * c
    tok = xbuf.shape[1]
    dim = kvb.shape[-1]
    chip = 2 * tok
    width = xbuf.shape[2]
    npair = w_hbm.shape[1]
    nq, nkv = npair // 2, npair // 4
    own = nq // 2

    def xor(p, m):
        hi, lo = p // 2, p - p // 2 * 2
        hi = 1 - hi if m >= 2 else hi
        lo = 1 - lo if m % 2 else lo
        return 2 * hi + lo

    def at(ra, rb, core):
        return (dp, rb * (1 - c) + ra * c, ra * (1 - c) + rb * c, core)

    def remote(src, dst, ssem, rsem, device):
        return pltpu.make_async_remote_copy(
            src_ref=src, dst_ref=dst, send_sem=ssem, recv_sem=rsem, device_id=device, device_id_type=MESH)

    def recv(dst, sem):
        remote(dst, dst, s_kv1.at[0], sem, at(a, b, 1 - c)).wait_recv()

    def rows_of(p, size):
        return pl.ds(pl.multiple_of(p * size, size), size)

    x_cp = pltpu.make_async_copy(x_hbm.at[0], xbuf.at[c], sem_x)
    x_cp.start()
    far_a, far_b = 1 - a // 2, 1 - b // 2
    steps = [(c, far_a), (1 - c, far_b), (c, 1 - far_a), (1 - c, 1 - far_b)]
    pairs = []
    for plane, q in steps:
        pairs += [nq + own // 2 * plane + q, nq + nkv + own // 2 * plane + q]
    for q in (far_a, 1 - far_a):
        pairs += [own * c + 2 * q, own * c + 2 * q + 1]
    w_cps = [pltpu.make_async_copy(w_hbm.at[:, p], wstage.at[i], sem_w.at[i]) for i, p in enumerate(pairs)]

    def fetch(i):
        w_cps[2 * i].start()
        w_cps[2 * i + 1].start()

    fetch(0)

    barrier = pltpu.get_barrier_semaphore()
    peers = [at(a, b, 1 - c)]
    for m in range(1, n):
        for core in (c, 1 - c):
            peers += [at(xor(a, m), b, core), at(a, xor(b, m), core)]
    for p in peers:
        pl.semaphore_signal(barrier, inc=1, device_id=p, device_id_type=MESH)

    er = lax.broadcasted_iota(jnp.int32, (dim, 4 * dim), 0)
    ec = lax.broadcasted_iota(jnp.int32, (dim, 4 * dim), 1)
    sel = jnp.where(ec < 2 * dim, 2 * er, 2 * dim + 2 * er + 1)
    spread = jnp.where(ec == sel, 1.0, 0.0).astype(BF16)

    def expand(core):
        nb = width // dim
        step = 4
        for j0 in range(0, nb, step):
            xs = jnp.concatenate([xbuf[core, :, (j0 + j) * dim:(j0 + j + 1) * dim] for j in range(step)], axis=0)
            r = jnp.dot(xs, spread, preferred_element_type=F32).astype(BF16)
            for j in range(step):
                cols = slice((j0 + j) * 2 * dim, (j0 + j + 1) * 2 * dim)
                for e in range(2):
                    xil[e, core, :, cols] = r[j * tok:(j + 1) * tok, e * 2 * dim:(e + 1) * 2 * dim]

    def weights(i):
        w_cps[2 * i].wait()
        w_cps[2 * i + 1].wait()
        return jnp.concatenate([wstage[2 * i].reshape(2 * width, dim), wstage[2 * i + 1].reshape(2 * width, dim)], axis=1)

    sends = []

    def start(cp):
        cp.start()
        sends.append(cp)

    def kv_dot(i):
        r = jnp.dot(xil[:, c].reshape(chip, 2 * width), weights(i), preferred_element_type=F32).astype(BF16)
        for e in range(2):
            for kv in range(2):
                kvout[2 * i + e, kv] = r[e * tok:(e + 1) * tok, kv * dim:(kv + 1) * dim]

    def kv_send(i):
        own_plane, place = i % 2 == 0, (a, b)[i % 2]
        for low in range(2):
            m = low + (2 if i < 2 else 0)
            e = xor(place, m) - xor(place, m) // 2 * 2
            where = rows_of(2 * m + c, tok)
            if own_plane and m == 0:
                kvb[0, :, where] = kvout[2 * i + e]
                continue
            device = at(xor(a, m), b, c) if own_plane else at(a, xor(b, m), 1 - c)
            start(remote(kvout.at[2 * i + e], kvb.at[0, :, where], s_kv1.at[2 * i + low], r_kv1.at[m, c], device))

    def q_dot(i):
        r = jnp.dot(xil[...].reshape(2 * chip, 2 * width), weights(4 + i), preferred_element_type=F32).astype(BF16)
        for e in range(2):
            for h in range(2):
                qout[2 * i + e, h] = r[h * chip:(h + 1) * chip, e * dim:(e + 1) * dim]

    def q_send(i):
        for low in range(2):
            m = low + (2 if i == 0 else 0)
            e = xor(a, m) - xor(a, m) // 2 * 2
            if m == 0:
                qb[0] = qout[2 * i + e]
            else:
                start(remote(qout.at[2 * i + e], qb.at[m], s_q1.at[m], r_q1.at[m], at(xor(a, m), b, c)))

    def forward(m):
        for core in (c, 1 - c):
            if m > 0 or core is not c:
                recv(kvb.at[0, :, rows_of(2 * m + core, tok)], r_kv1.at[m, core])
        part = rows_of(m, chip)
        for v in (1, 3):
            start(remote(kvb.at[0, :, part], kvb.at[v, :, part], s_kv2.at[v, m], r_kv2.at[v, m], at(a, xor(b, v), c)))

    x_cp.wait()
    fetch(1)
    fetch(2)
    expand(c)
    kv_dot(0)
    fetch(3)
    pl.semaphore_wait(barrier, len(peers))
    x_rc = remote(xbuf.at[c], xbuf.at[c], sx_send, sx_recv, at(a, b, 1 - c))
    x_rc.start()
    kv_send(0)
    kv_dot(1)
    fetch(4)
    kv_send(1)
    kv_dot(2)
    fetch(5)
    kv_send(2)
    kv_dot(3)
    kv_send(3)
    heads = [own * c + xor(a, m) for m in range(n)] + [own * (1 - c) + xor(b, m) for m in range(n)]
    wo_cps = [pltpu.make_async_copy(wo_hbm.at[g], wo.at[k], sem_wo.at[k]) for k, g in enumerate(heads)]
    x_rc.wait_recv()
    expand(1 - c)
    q_dot(0)
    q_send(0)
    forward(2)
    forward(3)
    q_dot(1)
    q_send(1)
    for cp in wo_cps:
        cp.start()
    forward(1)
    forward(0)

    scale = dim ** -0.5 * math.log2(math.e)
    keys = kvb.shape[2]

    def attend(block, tiles, first, last, then):
        def scores(t):
            return lax.dot_general(qb[t].reshape(2 * chip, dim), kvb[block, 0], (((1,), (1,)), ((), ())),
                                   preferred_element_type=F32)

        def finish(t, p, alpha, l):
            o = jnp.dot(p, kvb[block, 1], preferred_element_type=F32)
            if not first:
                o = acc[t] * alpha + o
            if last:
                o = (o / jnp.sum(l, axis=1, keepdims=True)).astype(BF16)
                osend[t] = o.reshape(2, chip, dim)
                then(t)
            else:
                acc[t] = o

        ahead, held = scores(tiles[0]), None
        for k, t in enumerate(tiles):
            s = ahead
            if k + 1 < len(tiles):
                ahead = scores(tiles[k + 1])
            top = s[:, :dim]
            for j in range(1, keys // dim):
                top = jnp.maximum(top, s[:, j * dim:(j + 1) * dim])
            top = jnp.broadcast_to(jnp.max(top, axis=1, keepdims=True), (2 * chip, dim))
            alpha = None
            if not first:
                old = mrun[t]
                top = jnp.maximum(top, old)
                alpha = jnp.exp2((old - top) * scale)
            p, l = [], None
            for j in range(keys // dim):
                pj = jnp.exp2((s[:, j * dim:(j + 1) * dim] - top) * scale)
                l = pj if l is None else l + pj
                p.append(pj.astype(BF16))
            if not first:
                l = lrun[t] * alpha + l
            if not last:
                mrun[t] = top
                lrun[t] = l
            if held is not None:
                finish(*held)
            held = (t, jnp.concatenate(p, axis=1), alpha, l)
        finish(*held)

    def from_side(v, m):
        recv(kvb.at[v, :, rows_of(m, chip)], r_kv2.at[v, m])

    def relay(v, m):
        part = rows_of(m, chip)
        start(remote(kvb.at[v, :, part], kvb.at[2, :, part], s_kv3.at[m], r_kv3.at[m], at(a, xor(b, 4 - v), c)))

    attend(0, (0,), True, False, None)
    for m in (2, 3, 1):
        recv(qb.at[m], r_q1.at[m])
    from_side(1, 2)
    relay(1, 2)
    from_side(3, 3)
    relay(3, 3)
    attend(0, (1, 2, 3), True, False, None)
    for m in (3, 1, 0):
        from_side(1, m)
    relay(1, 1)
    for m in (2, 1, 0):
        from_side(3, m)
    relay(3, 0)
    attend(1, (0, 1, 2, 3), False, False, None)
    attend(3, (0, 1, 2, 3), False, False, None)
    for m in range(n):
        recv(kvb.at[2, :, rows_of(m, chip)], r_kv3.at[m])

    def give_back(m):
        for e, core in enumerate((c, 1 - c)):
            part = rows_of(core, tok)
            if m == 0 and e == 0:
                orecv[0] = osend[0, :, part]
            else:
                start(remote(osend.at[m, :, part], orecv.at[n * e + m], s_o.at[m, e], r_o.at[n * e + m],
                             at(xor(a, m), b, core)))

    attend(2, (2, 3, 1, 0), False, True, give_back)

    for cp in wo_cps:
        cp.wait()
    yacc = None
    for k in (0, n, 2, n + 2, 3, n + 3, 1, n + 1):
        if k > 0:
            recv(orecv.at[k], r_o.at[k])
        o = jnp.concatenate([orecv[k, 0], orecv[k, 1]], axis=1)
        r = jnp.dot(o, wo[k], preferred_element_type=F32)
        yacc = r if yacc is None else yacc + r
    y_ref[0] = yacc.astype(BF16)

    x_rc.wait_send()
    for cp in sends:
        cp.wait_send()


def solution(mesh):
    n = mesh.shape["cx"]
    assert mesh.shape["cy"] == n and n == 4 and mesh.shape["core"] == 2
    seq_spec = P("dp", ("cy", "cx", "core"))

    def local_layer(x_loc, w_qkv, w_out):
        _, tok, width = x_loc.shape
        heads, dim, out_width = w_out.shape
        all_heads = w_qkv.shape[1]
        kv = (all_heads - heads) // 2
        assert kv == 2 * n and heads == 2 * kv
        chip = 2 * tok
        keys = n * chip
        w_pairs = w_qkv.reshape(width, all_heads // 2, 2, dim)
        wo_pairs = w_out.reshape(kv, 2 * dim, out_width)
        dma = pltpu.SemaphoreType.DMA
        return pl.pallas_call(
            functools.partial(kernel, n),
            out_shape=pltpu.VMEM(x_loc.shape, BF16),
            in_specs=[pl.BlockSpec(memory_space=pl.ANY)] * 3,
            out_specs=pl.BlockSpec(memory_space=pltpu.VMEM),
            scratch_shapes=[
                pltpu.VMEM((2, tok, width), BF16),
                pltpu.VMEM((2, 2, tok, 2 * width), BF16),
                pltpu.VMEM((kv + n, width, 2, dim), BF16),
                pltpu.VMEM((kv, 2 * dim, out_width), BF16),
                pltpu.VMEM((kv, 2, tok, dim), BF16),
                pltpu.VMEM((n, 2, chip, dim), BF16),
                pltpu.VMEM((4, 2, keys, dim), BF16),
                pltpu.VMEM((n, 2, chip, dim), BF16),
                pltpu.VMEM((n, 2 * chip, dim), F32),
                pltpu.VMEM((n, 2 * chip, dim), F32),
                pltpu.VMEM((n, 2 * chip, dim), F32),
                pltpu.VMEM((n, 2, chip, dim), BF16),
                pltpu.VMEM((kv, 2, tok, dim), BF16),
                dma, dma((kv + n,)), dma((kv,)),
                dma, dma,
                dma((kv,)), dma((n, 2)), dma((n,)), dma((n,)),
                dma((n, n)), dma((n, n)), dma((n,)), dma((n,)),
                dma((n, 2)), dma((kv,)),
            ],
            compiler_params=pltpu.CompilerParams(
                collective_id=0, has_side_effects=True, vmem_limit_bytes=58 * 1024 * 1024),
        )(x_loc, w_pairs, wo_pairs)

    return jax.shard_map(local_layer, mesh=mesh, in_specs=(seq_spec, P(), P()), out_specs=seq_spec, check_vma=False)
```

```python
import functools
import math

import jax
import jax.numpy as jnp
from jax import lax
from jax.experimental import pallas as pl
from jax.experimental.pallas import tpu as pltpu
from jax.sharding import PartitionSpec as P

MESH = pl.DeviceIdType.MESH
F32 = jnp.float32
BF16 = jnp.bfloat16


def kernel(n, x_hbm, w_hbm, wo_hbm, y_ref,
           xbuf, xil, wstage, wo, kvout, qout, kvb, qb, acc, mrun, lrun, osend, orecv,
           sem_x, sem_w, sem_wo, sx_send, sx_recv, s_kv1, r_kv1, s_q1, r_q1,
           s_kv2, r_kv2, s_kv3, r_kv3, s_o, r_o):
    dp = lax.axis_index("dp")
    cy = lax.axis_index("cy")
    cx = lax.axis_index("cx")
    c = lax.axis_index("core")
    a = cx * (1 - c) + cy * c
    b = cy * (1 - c) + cx * c
    tok = xbuf.shape[1]
    dim = kvb.shape[-1]
    chip = 2 * tok
    width = xbuf.shape[2]
    npair = w_hbm.shape[1]
    nq, nkv = npair // 2, npair // 4
    own = nq // 2

    def xor(p, m):
        hi, lo = p // 2, p - p // 2 * 2
        hi = 1 - hi if m >= 2 else hi
        lo = 1 - lo if m % 2 else lo
        return 2 * hi + lo

    def at(ra, rb, core):
        return (dp, rb * (1 - c) + ra * c, ra * (1 - c) + rb * c, core)

    def remote(src, dst, ssem, rsem, device):
        return pltpu.make_async_remote_copy(
            src_ref=src, dst_ref=dst, send_sem=ssem, recv_sem=rsem, device_id=device, device_id_type=MESH)

    def recv(dst, sem):
        remote(dst, dst, s_kv1.at[0], sem, at(a, b, 1 - c)).wait_recv()

    def rows_of(p, size):
        return pl.ds(pl.multiple_of(p * size, size), size)

    x_cp = pltpu.make_async_copy(x_hbm.at[0], xbuf.at[c], sem_x)
    x_cp.start()
    far_a, far_b = 1 - a // 2, 1 - b // 2
    steps = [(c, far_a), (1 - c, far_b), (c, 1 - far_a), (1 - c, 1 - far_b)]
    pairs = []
    for plane, q in steps:
        pairs += [nq + own // 2 * plane + q, nq + nkv + own // 2 * plane + q]
    for q in (far_a, 1 - far_a):
        pairs += [own * c + 2 * q, own * c + 2 * q + 1]
    w_cps = [pltpu.make_async_copy(w_hbm.at[:, p], wstage.at[i], sem_w.at[i]) for i, p in enumerate(pairs)]

    def fetch(i):
        w_cps[2 * i].start()
        w_cps[2 * i + 1].start()

    fetch(0)

    barrier = pltpu.get_barrier_semaphore()
    peers = [at(a, b, 1 - c)]
    for m in range(1, n):
        for core in (c, 1 - c):
            peers += [at(xor(a, m), b, core), at(a, xor(b, m), core)]
    for p in peers:
        pl.semaphore_signal(barrier, inc=1, device_id=p, device_id_type=MESH)

    lanes = 2 * dim
    copy = jnp.where(lax.broadcasted_iota(jnp.int32, (dim, lanes), 1) // 2
                     == lax.broadcasted_iota(jnp.int32, (dim, lanes), 0), 1.0, 0.0).astype(BF16)
    odd = lax.rem(lax.broadcasted_iota(jnp.int32, (tok, lanes), 1), 2)
    keep = [jnp.where(odd == e, 1.0, 0.0).astype(BF16) for e in range(2)]

    def expand(core):
        step = 4
        for j0 in range(0, width // dim, step):
            xs = jnp.concatenate([xbuf[core, :, (j0 + j) * dim:(j0 + j + 1) * dim] for j in range(step)], axis=0)
            r = jnp.dot(xs, copy, preferred_element_type=F32).astype(BF16)
            for j in range(step):
                for e in range(2):
                    xil[rows_of(2 * e + core, tok), (j0 + j) * lanes:(j0 + j + 1) * lanes] = \
                        r[j * tok:(j + 1) * tok] * keep[e]

    def weights(i):
        w_cps[2 * i].wait()
        w_cps[2 * i + 1].wait()
        return jnp.concatenate([wstage[2 * i].reshape(2 * width, dim), wstage[2 * i + 1].reshape(2 * width, dim)], axis=1)

    sends = []

    def start(cp):
        cp.start()
        sends.append(cp)

    def kv_dot(i):
        rows = jnp.concatenate([xil[rows_of(c, tok)], xil[rows_of(2 + c, tok)]], axis=0)
        r = jnp.dot(rows, weights(i), preferred_element_type=F32).astype(BF16)
        for e in range(2):
            for kv in range(2):
                kvout[2 * i + e, kv] = r[e * tok:(e + 1) * tok, kv * dim:(kv + 1) * dim]

    def kv_send(i):
        own_plane, place = i % 2 == 0, (a, b)[i % 2]
        for low in range(2):
            m = low + (2 if i < 2 else 0)
            e = xor(place, m) - xor(place, m) // 2 * 2
            where = rows_of(2 * m + c, tok)
            if own_plane and m == 0:
                kvb[0, :, where] = kvout[2 * i + e]
                continue
            device = at(xor(a, m), b, c) if own_plane else at(a, xor(b, m), 1 - c)
            start(remote(kvout.at[2 * i + e], kvb.at[0, :, where], s_kv1.at[2 * i + low], r_kv1.at[m, c], device))

    def q_dot(i):
        w = weights(4 + i)
        for h in range(2):
            r = jnp.dot(xil[h * chip:(h + 1) * chip], w, preferred_element_type=F32).astype(BF16)
            for e in range(2):
                qout[2 * i + e, h] = r[:, e * dim:(e + 1) * dim]

    def q_send(i):
        for low in range(2):
            m = low + (2 if i == 0 else 0)
            e = xor(a, m) - xor(a, m) // 2 * 2
            if m == 0:
                qb[0] = qout[2 * i + e]
            else:
                start(remote(qout.at[2 * i + e], qb.at[m], s_q1.at[m], r_q1.at[m], at(xor(a, m), b, c)))

    def forward(m):
        for core in (c, 1 - c):
            if m > 0 or core is not c:
                recv(kvb.at[0, :, rows_of(2 * m + core, tok)], r_kv1.at[m, core])
        part = rows_of(m, chip)
        for v in (1, 3):
            start(remote(kvb.at[0, :, part], kvb.at[v, :, part], s_kv2.at[v, m], r_kv2.at[v, m], at(a, xor(b, v), c)))

    x_cp.wait()
    fetch(1)
    fetch(2)
    expand(c)
    kv_dot(0)
    fetch(3)
    pl.semaphore_wait(barrier, len(peers))
    x_rcs = [remote(xil.at[rows_of(2 * e + c, tok)], xil.at[rows_of(2 * e + c, tok)], sx_send.at[e], sx_recv.at[e],
                    at(a, b, 1 - c)) for e in range(2)]
    for cp in x_rcs:
        start(cp)
    kv_send(0)
    kv_dot(1)
    fetch(4)
    kv_send(1)
    kv_dot(2)
    fetch(5)
    kv_send(2)
    kv_dot(3)
    kv_send(3)
    heads = [own * c + xor(a, m) for m in range(n)] + [own * (1 - c) + xor(b, m) for m in range(n)]
    wo_cps = [pltpu.make_async_copy(wo_hbm.at[g], wo.at[k], sem_wo.at[k]) for k, g in enumerate(heads)]
    for cp in x_rcs:
        cp.wait_recv()
    q_dot(0)
    q_send(0)
    q_dot(1)
    q_send(1)
    for cp in wo_cps:
        cp.start()
    forward(2)
    forward(3)
    forward(1)
    forward(0)

    scale = dim ** -0.5 * math.log2(math.e)
    keys = kvb.shape[2]

    def attend(items, then):
        def part(group, kv):
            if group in (0, 3):
                return kvb[0 if group == 0 else 2, kv]
            rows = slice(keys // 2, keys) if group == 1 else slice(0, keys // 2)
            return jnp.concatenate([kvb[1, kv, rows], kvb[3, kv, rows]], axis=0)

        def scores(group, t):
            return lax.dot_general(qb[t].reshape(2 * chip, dim), part(group, 0), (((1,), (1,)), ((), ())),
                                   preferred_element_type=F32)

        def finish(group, t, p, alpha, l):
            o = jnp.dot(p, part(group, 1), preferred_element_type=F32)
            if group != 0:
                o = acc[t] * alpha + o
            if group == 3:
                o = (o / jnp.sum(l, axis=1, keepdims=True)).astype(BF16)
                osend[t] = o.reshape(2, chip, dim)
                then(t)
            else:
                acc[t] = o

        ahead, held = scores(*items[0]), None
        for k, (group, t) in enumerate(items):
            s = ahead
            if k + 1 < len(items):
                ahead = scores(*items[k + 1])
            top = s[:, :dim]
            for j in range(1, keys // dim):
                top = jnp.maximum(top, s[:, j * dim:(j + 1) * dim])
            top = jnp.broadcast_to(jnp.max(top, axis=1, keepdims=True), (2 * chip, dim))
            alpha = None
            if group != 0:
                old = mrun[t]
                top = jnp.maximum(top, old)
                alpha = jnp.exp2((old - top) * scale)
            p, l = [], None
            for j in range(keys // dim):
                pj = jnp.exp2((s[:, j * dim:(j + 1) * dim] - top) * scale)
                l = pj if l is None else l + pj
                p.append(pj.astype(BF16))
            if group != 0:
                l = lrun[t] * alpha + l
            if group != 3:
                mrun[t] = top
                lrun[t] = l
            if held is not None:
                finish(*held)
            held = (group, t, jnp.concatenate(p, axis=1), alpha, l)
        finish(*held)

    def from_side(v, m):
        recv(kvb.at[v, :, rows_of(m, chip)], r_kv2.at[v, m])

    def relay(v, m):
        part = rows_of(m, chip)
        start(remote(kvb.at[v, :, part], kvb.at[2, :, part], s_kv3.at[m], r_kv3.at[m], at(a, xor(b, 4 - v), c)))

    attend([(0, 0)], None)
    for v, m in ((1, 2), (3, 3)):
        from_side(v, m)
        relay(v, m)
    for v, m in ((1, 3), (3, 2)):
        from_side(v, m)
    attend([(1, 0)], None)
    for m in (2, 3, 1):
        recv(qb.at[m], r_q1.at[m])
    attend([(0, 1), (0, 2), (0, 3), (1, 1)], None)
    for v, m in ((1, 1), (3, 0)):
        from_side(v, m)
        relay(v, m)
    attend([(1, 2), (1, 3)], None)
    for v, m in ((1, 0), (3, 1)):
        from_side(v, m)
    attend([(2, t) for t in range(n)], None)
    for m in range(n):
        recv(kvb.at[2, :, rows_of(m, chip)], r_kv3.at[m])

    def give_back(m):
        for e, core in enumerate((c, 1 - c)):
            part = rows_of(core, tok)
            if m == 0 and e == 0:
                orecv[0] = osend[0, :, part]
            else:
                start(remote(osend.at[m, :, part], orecv.at[n * e + m], s_o.at[m, e], r_o.at[n * e + m],
                             at(xor(a, m), b, core)))

    attend([(3, 2), (3, 3), (3, 1), (3, 0)], give_back)

    for cp in wo_cps:
        cp.wait()
    yacc = None
    for k in (0, 2, n + 2, 3, n + 3, n, 1, n + 1):
        if k > 0:
            recv(orecv.at[k], r_o.at[k])
        o = jnp.concatenate([orecv[k, 0], orecv[k, 1]], axis=1)
        r = jnp.dot(o, wo[k], preferred_element_type=F32)
        yacc = r if yacc is None else yacc + r
    y_ref[0] = yacc.astype(BF16)

    for cp in sends:
        cp.wait_send()


def solution(mesh):
    n = mesh.shape["cx"]
    assert mesh.shape["cy"] == n and n == 4 and mesh.shape["core"] == 2
    seq_spec = P("dp", ("cy", "cx", "core"))

    def local_layer(x_loc, w_qkv, w_out):
        _, tok, width = x_loc.shape
        heads, dim, out_width = w_out.shape
        all_heads = w_qkv.shape[1]
        kv = (all_heads - heads) // 2
        assert kv == 2 * n and heads == 2 * kv
        chip = 2 * tok
        keys = n * chip
        w_pairs = w_qkv.reshape(width, all_heads // 2, 2, dim)
        wo_pairs = w_out.reshape(kv, 2 * dim, out_width)
        dma = pltpu.SemaphoreType.DMA
        return pl.pallas_call(
            functools.partial(kernel, n),
            out_shape=pltpu.VMEM(x_loc.shape, BF16),
            in_specs=[pl.BlockSpec(memory_space=pl.ANY)] * 3,
            out_specs=pl.BlockSpec(memory_space=pltpu.VMEM),
            scratch_shapes=[
                pltpu.VMEM((2, tok, width), BF16),
                pltpu.VMEM((2 * chip, 2 * width), BF16),
                pltpu.VMEM((kv + n, width, 2, dim), BF16),
                pltpu.VMEM((kv, 2 * dim, out_width), BF16),
                pltpu.VMEM((kv, 2, tok, dim), BF16),
                pltpu.VMEM((n, 2, chip, dim), BF16),
                pltpu.VMEM((4, 2, keys, dim), BF16),
                pltpu.VMEM((n, 2, chip, dim), BF16),
                pltpu.VMEM((n, 2 * chip, dim), F32),
                pltpu.VMEM((n, 2 * chip, dim), F32),
                pltpu.VMEM((n, 2 * chip, dim), F32),
                pltpu.VMEM((n, 2, chip, dim), BF16),
                pltpu.VMEM((kv, 2, tok, dim), BF16),
                dma, dma((kv + n,)), dma((kv,)),
                dma((2,)), dma((2,)),
                dma((kv,)), dma((n, 2)), dma((n,)), dma((n,)),
                dma((n, n)), dma((n, n)), dma((n,)), dma((n,)),
                dma((n, 2)), dma((kv,)),
            ],
            compiler_params=pltpu.CompilerParams(
                collective_id=0, has_side_effects=True, vmem_limit_bytes=58 * 1024 * 1024),
        )(x_loc, w_pairs, wo_pairs)

    return jax.shard_map(local_layer, mesh=mesh, in_specs=(seq_spec, P(), P()), out_specs=seq_spec, check_vma=False)
```

```python
import functools
import math

import jax
import jax.numpy as jnp
from jax import lax
from jax.experimental import pallas as pl
from jax.experimental.pallas import tpu as pltpu
from jax.sharding import PartitionSpec as P

MESH = pl.DeviceIdType.MESH
F32 = jnp.float32
BF16 = jnp.bfloat16


def kernel(n, x_hbm, w_hbm, wo_hbm, y_ref,
           xbuf, xil, wstage, wo, kvout, qout, kvb, qb, acc, mrun, lrun, osend, orecv,
           sem_x, sem_w, sem_wo, sx_send, sx_recv, s_kv1, r_kv1, s_q1, r_q1,
           s_kv2, r_kv2, s_kv3, s_o, r_o):
    dp = lax.axis_index("dp")
    cy = lax.axis_index("cy")
    cx = lax.axis_index("cx")
    c = lax.axis_index("core")
    a = cx * (1 - c) + cy * c
    b = cy * (1 - c) + cx * c
    tok = xbuf.shape[1]
    dim = kvb.shape[-1]
    chip = 2 * tok
    width = xbuf.shape[2]
    npair = w_hbm.shape[1]
    nq, nkv = npair // 2, npair // 4
    own = nq // 2

    def xor(p, m):
        hi, lo = p // 2, p - p // 2 * 2
        hi = 1 - hi if m >= 2 else hi
        lo = 1 - lo if m % 2 else lo
        return 2 * hi + lo

    def at(ra, rb, core):
        return (dp, rb * (1 - c) + ra * c, ra * (1 - c) + rb * c, core)

    def remote(src, dst, ssem, rsem, device):
        return pltpu.make_async_remote_copy(
            src_ref=src, dst_ref=dst, send_sem=ssem, recv_sem=rsem, device_id=device, device_id_type=MESH)

    def recv(dst, sem):
        remote(dst, dst, s_kv1.at[0], sem, at(a, b, 1 - c)).wait_recv()

    def rows_of(p, size):
        return pl.ds(pl.multiple_of(p * size, size), size)

    turn = {0: 0, 2: 1, 3: 2, 1: 3}

    def spot(m):
        return pl.ds(turn[m] * chip, chip)

    x_cp = pltpu.make_async_copy(x_hbm.at[0], xbuf.at[c], sem_x)
    x_cp.start()
    far_a, far_b = 1 - a // 2, 1 - b // 2
    steps = [(c, far_a), (1 - c, far_b), (c, 1 - far_a), (1 - c, 1 - far_b)]
    pairs = []
    for plane, q in steps:
        pairs += [nq + own // 2 * plane + q, nq + nkv + own // 2 * plane + q]
    for q in (far_a, 1 - far_a):
        pairs += [own * c + 2 * q, own * c + 2 * q + 1]
    w_cps = [pltpu.make_async_copy(w_hbm.at[:, p], wstage.at[i], sem_w.at[i]) for i, p in enumerate(pairs)]

    def fetch(i):
        w_cps[2 * i].start()
        w_cps[2 * i + 1].start()

    fetch(0)

    barrier = pltpu.get_barrier_semaphore()
    peers = [at(a, b, 1 - c)]
    for m in range(1, n):
        for core in (c, 1 - c):
            peers += [at(xor(a, m), b, core), at(a, xor(b, m), core)]
    for p in peers:
        pl.semaphore_signal(barrier, inc=1, device_id=p, device_id_type=MESH)

    lanes = 2 * dim
    copy = jnp.where(lax.broadcasted_iota(jnp.int32, (dim, lanes), 1) // 2
                     == lax.broadcasted_iota(jnp.int32, (dim, lanes), 0), 1.0, 0.0).astype(BF16)
    odd = lax.rem(lax.broadcasted_iota(jnp.int32, (tok, lanes), 1), 2)
    keep = [jnp.where(odd == e, 1.0, 0.0).astype(BF16) for e in range(2)]

    def expand(core):
        step = 4
        for j0 in range(0, width // dim, step):
            xs = jnp.concatenate([xbuf[core, :, (j0 + j) * dim:(j0 + j + 1) * dim] for j in range(step)], axis=0)
            r = jnp.dot(xs, copy, preferred_element_type=F32).astype(BF16)
            for j in range(step):
                for e in range(2):
                    xil[rows_of(2 * e + core, tok), (j0 + j) * lanes:(j0 + j + 1) * lanes] = \
                        r[j * tok:(j + 1) * tok] * keep[e]

    def weights(i):
        w_cps[2 * i].wait()
        w_cps[2 * i + 1].wait()
        return jnp.concatenate([wstage[2 * i].reshape(2 * width, dim), wstage[2 * i + 1].reshape(2 * width, dim)], axis=1)

    sends = []

    def start(cp):
        cp.start()
        sends.append(cp)

    def kv_dot(i):
        rows = jnp.concatenate([xil[rows_of(c, tok)], xil[rows_of(2 + c, tok)]], axis=0)
        r = jnp.dot(rows, weights(i), preferred_element_type=F32).astype(BF16)
        for e in range(2):
            for kv in range(2):
                kvout[2 * i + e, kv] = r[e * tok:(e + 1) * tok, kv * dim:(kv + 1) * dim]

    def kv_send(i):
        own_plane, place = i % 2 == 0, (a, b)[i % 2]
        for low in range(2):
            m = low + (2 if i < 2 else 0)
            e = xor(place, m) - xor(place, m) // 2 * 2
            where = rows_of(2 * turn[m] + c, tok)
            if own_plane and m == 0:
                kvb[0, :, where] = kvout[2 * i + e]
                continue
            device = at(xor(a, m), b, c) if own_plane else at(a, xor(b, m), 1 - c)
            start(remote(kvout.at[2 * i + e], kvb.at[0, :, where], s_kv1.at[2 * i + low], r_kv1.at[m, c], device))

    def q_dot(i):
        w = weights(4 + i)
        for h in range(2):
            r = jnp.dot(xil[h * chip:(h + 1) * chip], w, preferred_element_type=F32).astype(BF16)
            for e in range(2):
                qout[2 * i + e, h] = r[:, e * dim:(e + 1) * dim]

    def q_send(i):
        for low in range(2):
            m = low + (2 if i == 0 else 0)
            e = xor(a, m) - xor(a, m) // 2 * 2
            if m == 0:
                qb[0] = qout[2 * i + e]
            else:
                start(remote(qout.at[2 * i + e], qb.at[m], s_q1.at[m], r_q1.at[m], at(xor(a, m), b, c)))

    def onward(m, v):
        part = spot(m)
        start(remote(kvb.at[0, :, part], kvb.at[v, :, part], s_kv2.at[v, m], r_kv2.at[v, m], at(a, xor(b, v), c)))

    def forward(m):
        for core in (c, 1 - c):
            if m > 0 or core is not c:
                recv(kvb.at[0, :, rows_of(2 * turn[m] + core, tok)], r_kv1.at[m, core])
        onward(m, 1)
        onward(m, 3)

    x_cp.wait()
    fetch(1)
    fetch(2)
    expand(c)
    kv_dot(0)
    fetch(3)
    pl.semaphore_wait(barrier, len(peers))
    x_rcs = [remote(xil.at[rows_of(2 * e + c, tok)], xil.at[rows_of(2 * e + c, tok)], sx_send.at[e], sx_recv.at[e],
                    at(a, b, 1 - c)) for e in range(2)]
    for cp in x_rcs:
        start(cp)
    kv_send(0)
    kv_dot(1)
    fetch(4)
    kv_send(1)
    kv_dot(2)
    fetch(5)
    kv_send(2)
    kv_dot(3)
    kv_send(3)
    heads = [own * c + xor(a, m) for m in range(n)] + [own * (1 - c) + xor(b, m) for m in range(n)]
    wo_cps = [pltpu.make_async_copy(wo_hbm.at[g], wo.at[k], sem_wo.at[k]) for k, g in enumerate(heads)]
    for cp in x_rcs:
        cp.wait_recv()
    q_dot(0)
    q_send(0)
    forward(0)
    q_dot(1)
    q_send(1)
    for cp in wo_cps:
        cp.start()
    forward(2)
    forward(3)
    forward(1)
    onward(3, 2)
    onward(1, 2)

    scale = dim ** -0.5 * math.log2(math.e)
    keys = kvb.shape[2]

    def attend(items, then):
        def part(group, kv):
            if group in (0, 3):
                return kvb[0 if group == 0 else 2, kv]
            rows = slice(0, keys // 2) if group == 1 else slice(keys // 2, keys)
            return jnp.concatenate([kvb[1, kv, rows], kvb[3, kv, rows]], axis=0)

        def scores(group, t):
            return lax.dot_general(qb[t].reshape(2 * chip, dim), part(group, 0), (((1,), (1,)), ((), ())),
                                   preferred_element_type=F32)

        def finish(group, t, p, alpha, l):
            o = jnp.dot(p, part(group, 1), preferred_element_type=F32)
            if group != 0:
                o = acc[t] * alpha + o
            if group == 3:
                o = (o / jnp.sum(l, axis=1, keepdims=True)).astype(BF16)
                osend[t] = o.reshape(2, chip, dim)
                then(t)
            else:
                acc[t] = o

        ahead, held = scores(*items[0]), None
        for k, (group, t) in enumerate(items):
            s = ahead
            if k + 1 < len(items):
                ahead = scores(*items[k + 1])
            top = s[:, :dim]
            for j in range(1, keys // dim):
                top = jnp.maximum(top, s[:, j * dim:(j + 1) * dim])
            top = jnp.broadcast_to(jnp.max(top, axis=1, keepdims=True), (2 * chip, dim))
            alpha = None
            if group != 0:
                old = mrun[t]
                top = jnp.maximum(top, old)
                alpha = jnp.exp2((old - top) * scale)
            p, l = [], None
            for j in range(keys // dim):
                pj = jnp.exp2((s[:, j * dim:(j + 1) * dim] - top) * scale)
                l = pj if l is None else l + pj
                p.append(pj.astype(BF16))
            if group != 0:
                l = lrun[t] * alpha + l
            if group != 3:
                mrun[t] = top
                lrun[t] = l
            if held is not None:
                finish(*held)
            held = (group, t, jnp.concatenate(p, axis=1), alpha, l)
        finish(*held)

    def from_side(v, m):
        recv(kvb.at[v, :, spot(m)], r_kv2.at[v, m])

    def relay(v, m):
        part = spot(m)
        start(remote(kvb.at[v, :, part], kvb.at[2, :, part], s_kv3.at[m], r_kv2.at[2, m], at(a, xor(b, 4 - v), c)))

    attend([(0, 0)], None)
    from_side(1, 0)
    relay(1, 0)
    for m in (2, 3, 1):
        recv(qb.at[m], r_q1.at[m])
    attend([(0, 1), (0, 2), (0, 3)], None)
    from_side(3, 2)
    relay(3, 2)
    from_side(1, 2)
    from_side(3, 0)
    attend([(1, t) for t in range(n)], None)
    for v, m in ((1, 3), (3, 3), (1, 1), (3, 1)):
        from_side(v, m)
    attend([(2, t) for t in range(n)], None)
    for m in (0, 2, 3, 1):
        from_side(2, m)

    def give_back(m):
        for e, core in enumerate((c, 1 - c)):
            part = rows_of(core, tok)
            if m == 0 and e == 0:
                orecv[0] = osend[0, :, part]
            else:
                start(remote(osend.at[m, :, part], orecv.at[n * e + m], s_o.at[m, e], r_o.at[n * e + m],
                             at(xor(a, m), b, core)))

    attend([(3, 2), (3, 3), (3, 1), (3, 0)], give_back)

    for cp in wo_cps:
        cp.wait()
    yacc = None
    for k in (0, n, 1, 3, 2, n + 1, n + 3, n + 2):
        if k > 0:
            recv(orecv.at[k], r_o.at[k])
        o = jnp.concatenate([orecv[k, 0], orecv[k, 1]], axis=1)
        r = jnp.dot(o, wo[k], preferred_element_type=F32)
        yacc = r if yacc is None else yacc + r
    y_ref[0] = yacc.astype(BF16)

    for cp in sends:
        cp.wait_send()


def solution(mesh):
    n = mesh.shape["cx"]
    assert mesh.shape["cy"] == n and n == 4 and mesh.shape["core"] == 2
    seq_spec = P("dp", ("cy", "cx", "core"))

    def local_layer(x_loc, w_qkv, w_out):
        _, tok, width = x_loc.shape
        heads, dim, out_width = w_out.shape
        all_heads = w_qkv.shape[1]
        kv = (all_heads - heads) // 2
        assert kv == 2 * n and heads == 2 * kv
        chip = 2 * tok
        keys = n * chip
        w_pairs = w_qkv.reshape(width, all_heads // 2, 2, dim)
        wo_pairs = w_out.reshape(kv, 2 * dim, out_width)
        dma = pltpu.SemaphoreType.DMA
        return pl.pallas_call(
            functools.partial(kernel, n),
            out_shape=pltpu.VMEM(x_loc.shape, BF16),
            in_specs=[pl.BlockSpec(memory_space=pl.ANY)] * 3,
            out_specs=pl.BlockSpec(memory_space=pltpu.VMEM),
            scratch_shapes=[
                pltpu.VMEM((2, tok, width), BF16),
                pltpu.VMEM((2 * chip, 2 * width), BF16),
                pltpu.VMEM((kv + n, width, 2, dim), BF16),
                pltpu.VMEM((kv, 2 * dim, out_width), BF16),
                pltpu.VMEM((kv, 2, tok, dim), BF16),
                pltpu.VMEM((n, 2, chip, dim), BF16),
                pltpu.VMEM((4, 2, keys, dim), BF16),
                pltpu.VMEM((n, 2, chip, dim), BF16),
                pltpu.VMEM((n, 2 * chip, dim), F32),
                pltpu.VMEM((n, 2 * chip, dim), F32),
                pltpu.VMEM((n, 2 * chip, dim), F32),
                pltpu.VMEM((n, 2, chip, dim), BF16),
                pltpu.VMEM((kv, 2, tok, dim), BF16),
                dma, dma((kv + n,)), dma((kv,)),
                dma((2,)), dma((2,)),
                dma((kv,)), dma((n, 2)), dma((n,)), dma((n,)),
                dma((n, n)), dma((n, n)), dma((n,)),
                dma((n, 2)), dma((kv,)),
            ],
            compiler_params=pltpu.CompilerParams(
                collective_id=0, has_side_effects=True, vmem_limit_bytes=58 * 1024 * 1024),
        )(x_loc, w_pairs, wo_pairs)

    return jax.shard_map(local_layer, mesh=mesh, in_specs=(seq_spec, P(), P()), out_specs=seq_spec, check_vma=False)
```

```python
import functools
import math

import jax
import jax.numpy as jnp
from jax import lax
from jax.experimental import pallas as pl
from jax.experimental.pallas import tpu as pltpu
from jax.sharding import PartitionSpec as P

MESH = pl.DeviceIdType.MESH
F32 = jnp.float32
BF16 = jnp.bfloat16


def kernel(n, x_hbm, w_hbm, wo_hbm, y_ref,
           xbuf, xil, wstage, wo, kvout, qout, kvb, qb, acc, mrun, lrun, osend, orecv,
           sem_x, sem_w, sem_wo, sx_send, sx_recv, s_kv1, r_kv1, s_q1, r_q1,
           s_kv2, r_kv2, s_kv3, s_o, r_o):
    dp = lax.axis_index("dp")
    cy = lax.axis_index("cy")
    cx = lax.axis_index("cx")
    c = lax.axis_index("core")
    a = cx * (1 - c) + cy * c
    b = cy * (1 - c) + cx * c
    tok = xbuf.shape[1]
    dim = kvb.shape[-1]
    chip = 2 * tok
    width = xbuf.shape[2]
    npair = w_hbm.shape[1]
    nq, nkv = npair // 2, npair // 4
    own = nq // 2

    def xor(p, m):
        hi, lo = p // 2, p - p // 2 * 2
        hi = 1 - hi if m >= 2 else hi
        lo = 1 - lo if m % 2 else lo
        return 2 * hi + lo

    def at(ra, rb, core):
        return (dp, rb * (1 - c) + ra * c, ra * (1 - c) + rb * c, core)

    def remote(src, dst, ssem, rsem, device):
        return pltpu.make_async_remote_copy(
            src_ref=src, dst_ref=dst, send_sem=ssem, recv_sem=rsem, device_id=device, device_id_type=MESH)

    def recv(dst, sem):
        remote(dst, dst, s_kv1.at[0], sem, at(a, b, 1 - c)).wait_recv()

    def rows_of(p, size):
        return pl.ds(pl.multiple_of(p * size, size), size)

    turn = {0: 0, 2: 1, 3: 2, 1: 3}

    def spot(m):
        return pl.ds(turn[m] * chip, chip)

    x_cp = pltpu.make_async_copy(x_hbm.at[0], xbuf.at[c], sem_x)
    x_cp.start()
    far_a, far_b = 1 - a // 2, 1 - b // 2
    steps = [(c, far_a), (1 - c, far_b), (c, 1 - far_a), (1 - c, 1 - far_b)]
    pairs = []
    for plane, q in steps:
        pairs += [nq + own // 2 * plane + q, nq + nkv + own // 2 * plane + q]
    for q in (far_a, 1 - far_a):
        pairs += [own * c + 2 * q, own * c + 2 * q + 1]
    w_cps = [pltpu.make_async_copy(w_hbm.at[:, p], wstage.at[i], sem_w.at[i]) for i, p in enumerate(pairs)]

    def fetch(i):
        w_cps[2 * i].start()
        w_cps[2 * i + 1].start()

    fetch(0)

    barrier = pltpu.get_barrier_semaphore()
    peers = [at(a, b, 1 - c)]
    for m in range(1, n):
        for core in (c, 1 - c):
            peers += [at(xor(a, m), b, core), at(a, xor(b, m), core)]
    for p in peers:
        pl.semaphore_signal(barrier, inc=1, device_id=p, device_id_type=MESH)

    lanes = 2 * dim
    copy = jnp.where(lax.broadcasted_iota(jnp.int32, (dim, lanes), 1) // 2
                     == lax.broadcasted_iota(jnp.int32, (dim, lanes), 0), 1.0, 0.0).astype(BF16)
    odd = lax.rem(lax.broadcasted_iota(jnp.int32, (tok, lanes), 1), 2)
    keep = [jnp.where(odd == e, 1.0, 0.0).astype(BF16) for e in range(2)]

    def expand(core):
        step = 4
        for j0 in range(0, width // dim, step):
            xs = jnp.concatenate([xbuf[core, :, (j0 + j) * dim:(j0 + j + 1) * dim] for j in range(step)], axis=0)
            r = jnp.dot(xs, copy, preferred_element_type=F32).astype(BF16)
            for j in range(step):
                for e in range(2):
                    xil[rows_of(2 * e + core, tok), (j0 + j) * lanes:(j0 + j + 1) * lanes] = \
                        r[j * tok:(j + 1) * tok] * keep[e]

    def weights(i):
        w_cps[2 * i].wait()
        w_cps[2 * i + 1].wait()
        return jnp.concatenate([wstage[2 * i].reshape(2 * width, dim), wstage[2 * i + 1].reshape(2 * width, dim)], axis=1)

    sends = []

    def start(cp):
        cp.start()
        sends.append(cp)

    def kv_dot(i):
        rows = jnp.concatenate([xil[rows_of(c, tok)], xil[rows_of(2 + c, tok)]], axis=0)
        r = jnp.dot(rows, weights(i), preferred_element_type=F32).astype(BF16)
        for e in range(2):
            for kv in range(2):
                kvout[2 * i + e, kv] = r[e * tok:(e + 1) * tok, kv * dim:(kv + 1) * dim]

    def kv_send(i):
        own_plane, place = i % 2 == 0, (a, b)[i % 2]
        for low in range(2):
            m = low + (2 if i < 2 else 0)
            e = xor(place, m) - xor(place, m) // 2 * 2
            where = rows_of(2 * turn[m] + c, tok)
            if own_plane and m == 0:
                kvb[0, :, where] = kvout[2 * i + e]
                continue
            device = at(xor(a, m), b, c) if own_plane else at(a, xor(b, m), 1 - c)
            start(remote(kvout.at[2 * i + e], kvb.at[0, :, where], s_kv1.at[2 * i + low], r_kv1.at[m, c], device))

    def q_dot(i):
        w = weights(4 + i)
        for h in range(2):
            r = jnp.dot(xil[h * chip:(h + 1) * chip], w, preferred_element_type=F32).astype(BF16)
            for e in range(2):
                qout[2 * i + e, h] = r[:, e * dim:(e + 1) * dim]

    def q_send(i):
        for low in range(2):
            m = low + (2 if i == 0 else 0)
            e = xor(a, m) - xor(a, m) // 2 * 2
            if m == 0:
                qb[0] = qout[2 * i + e]
            else:
                start(remote(qout.at[2 * i + e], qb.at[m], s_q1.at[m], r_q1.at[m], at(xor(a, m), b, c)))

    def onward(m, v):
        part = spot(m)
        start(remote(kvb.at[0, :, part], kvb.at[v, :, part], s_kv2.at[v, m], r_kv2.at[v, m], at(a, xor(b, v), c)))

    def forward(m):
        for core in (c, 1 - c):
            if m > 0 or core is not c:
                recv(kvb.at[0, :, rows_of(2 * turn[m] + core, tok)], r_kv1.at[m, core])
        onward(m, 1)
        onward(m, 3)

    x_cp.wait()
    fetch(1)
    fetch(2)
    expand(c)
    kv_dot(0)
    fetch(3)
    pl.semaphore_wait(barrier, len(peers))
    x_rcs = [remote(xil.at[rows_of(2 * e + c, tok)], xil.at[rows_of(2 * e + c, tok)], sx_send.at[e], sx_recv.at[e],
                    at(a, b, 1 - c)) for e in range(2)]
    for cp in x_rcs:
        start(cp)
    kv_send(0)
    kv_dot(1)
    fetch(4)
    kv_send(1)
    kv_dot(2)
    fetch(5)
    kv_send(2)
    kv_dot(3)
    kv_send(3)
    heads = [own * c + xor(a, m) for m in range(n)] + [own * (1 - c) + xor(b, m) for m in range(n)]
    wo_cps = [pltpu.make_async_copy(wo_hbm.at[g], wo.at[k], sem_wo.at[k]) for k, g in enumerate(heads)]
    for cp in x_rcs:
        cp.wait_recv()
    q_dot(0)
    q_send(0)
    forward(0)
    q_dot(1)
    q_send(1)
    for cp in wo_cps:
        cp.start()
    forward(2)
    forward(3)
    forward(1)
    onward(3, 2)
    onward(1, 2)

    scale = dim ** -0.5 * math.log2(math.e)
    keys = kvb.shape[2]

    def attend(items, then):
        def part(group, kv):
            if group in (0, 3):
                return kvb[0 if group == 0 else 2, kv]
            rows = slice(0, keys // 2) if group == 1 else slice(keys // 2, keys)
            return jnp.concatenate([kvb[1, kv, rows], kvb[3, kv, rows]], axis=0)

        def scores(group, t):
            return lax.dot_general(qb[t].reshape(2 * chip, dim), part(group, 0), (((1,), (1,)), ((), ())),
                                   preferred_element_type=F32)

        def finish(group, t, p, alpha, l):
            o = jnp.dot(p, part(group, 1), preferred_element_type=F32)
            if group != 0:
                o = acc[t] * alpha + o
            if group == 3:
                o = (o / jnp.sum(l, axis=1, keepdims=True)).astype(BF16)
                osend[t] = o.reshape(2, chip, dim)
                then(t)
            else:
                acc[t] = o

        ahead, held = scores(*items[0]), None
        for k, (group, t) in enumerate(items):
            s = ahead
            if k + 1 < len(items):
                ahead = scores(*items[k + 1])
            top = s[:, :dim]
            for j in range(1, keys // dim):
                top = jnp.maximum(top, s[:, j * dim:(j + 1) * dim])
            top = jnp.broadcast_to(jnp.max(top, axis=1, keepdims=True), (2 * chip, dim))
            alpha = None
            if group != 0:
                old = mrun[t]
                top = jnp.maximum(top, old)
                alpha = jnp.exp2((old - top) * scale)
            p, l = [], None
            for j in range(keys // dim):
                pj = jnp.exp2((s[:, j * dim:(j + 1) * dim] - top) * scale)
                l = pj if l is None else l + pj
                p.append(pj.astype(BF16))
            if group != 0:
                l = lrun[t] * alpha + l
            if group != 3:
                mrun[t] = top
                lrun[t] = l
            if held is not None:
                finish(*held)
            held = (group, t, jnp.concatenate(p, axis=1), alpha, l)
        finish(*held)

    def from_side(v, m):
        recv(kvb.at[v, :, spot(m)], r_kv2.at[v, m])

    def relay(v, m):
        part = spot(m)
        start(remote(kvb.at[v, :, part], kvb.at[2, :, part], s_kv3.at[m], r_kv2.at[2, m], at(a, xor(b, 4 - v), c)))

    attend([(0, 0)], None)
    from_side(1, 0)
    relay(1, 0)
    for m in (2, 3, 1):
        recv(qb.at[m], r_q1.at[m])
    attend([(0, 1), (0, 2), (0, 3)], None)
    from_side(3, 2)
    relay(3, 2)
    from_side(1, 2)
    from_side(3, 0)
    attend([(1, t) for t in range(n)], None)
    for v, m in ((1, 3), (3, 3), (1, 1), (3, 1)):
        from_side(v, m)
    attend([(2, t) for t in range(n)], None)
    for m in (0, 2, 3, 1):
        from_side(2, m)

    def give_back(m):
        for e, core in enumerate((c, 1 - c)):
            part = rows_of(core, tok)
            if m == 0 and e == 0:
                orecv[0] = osend[0, :, part]
            else:
                start(remote(osend.at[m, :, part], orecv.at[n * e + m], s_o.at[m, e], r_o.at[n * e + m],
                             at(xor(a, m), b, core)))

    attend([(3, 3), (3, 2), (3, 1), (3, 0)], give_back)

    for cp in wo_cps:
        cp.wait()
    yacc = None
    for k in (0, n, 1, 2, n + 1, n + 2, 3, n + 3):
        if k > 0:
            recv(orecv.at[k], r_o.at[k])
        o = jnp.concatenate([orecv[k, 0], orecv[k, 1]], axis=1)
        r = jnp.dot(o, wo[k], preferred_element_type=F32)
        yacc = r if yacc is None else yacc + r
    y_ref[0] = yacc.astype(BF16)

    for cp in sends:
        cp.wait_send()


def solution(mesh):
    n = mesh.shape["cx"]
    assert mesh.shape["cy"] == n and n == 4 and mesh.shape["core"] == 2
    seq_spec = P("dp", ("cy", "cx", "core"))

    def local_layer(x_loc, w_qkv, w_out):
        _, tok, width = x_loc.shape
        heads, dim, out_width = w_out.shape
        all_heads = w_qkv.shape[1]
        kv = (all_heads - heads) // 2
        assert kv == 2 * n and heads == 2 * kv
        chip = 2 * tok
        keys = n * chip
        w_pairs = w_qkv.reshape(width, all_heads // 2, 2, dim)
        wo_pairs = w_out.reshape(kv, 2 * dim, out_width)
        dma = pltpu.SemaphoreType.DMA
        return pl.pallas_call(
            functools.partial(kernel, n),
            out_shape=pltpu.VMEM(x_loc.shape, BF16),
            in_specs=[pl.BlockSpec(memory_space=pl.ANY)] * 3,
            out_specs=pl.BlockSpec(memory_space=pltpu.VMEM),
            scratch_shapes=[
                pltpu.VMEM((2, tok, width), BF16),
                pltpu.VMEM((2 * chip, 2 * width), BF16),
                pltpu.VMEM((kv + n, width, 2, dim), BF16),
                pltpu.VMEM((kv, 2 * dim, out_width), BF16),
                pltpu.VMEM((kv, 2, tok, dim), BF16),
                pltpu.VMEM((n, 2, chip, dim), BF16),
                pltpu.VMEM((4, 2, keys, dim), BF16),
                pltpu.VMEM((n, 2, chip, dim), BF16),
                pltpu.VMEM((n, 2 * chip, dim), F32),
                pltpu.VMEM((n, 2 * chip, dim), F32),
                pltpu.VMEM((n, 2 * chip, dim), F32),
                pltpu.VMEM((n, 2, chip, dim), BF16),
                pltpu.VMEM((kv, 2, tok, dim), BF16),
                dma, dma((kv + n,)), dma((kv,)),
                dma((2,)), dma((2,)),
                dma((kv,)), dma((n, 2)), dma((n,)), dma((n,)),
                dma((n, n)), dma((n, n)), dma((n,)),
                dma((n, 2)), dma((kv,)),
            ],
            compiler_params=pltpu.CompilerParams(
                collective_id=0, has_side_effects=True, vmem_limit_bytes=58 * 1024 * 1024),
        )(x_loc, w_pairs, wo_pairs)

    return jax.shard_map(local_layer, mesh=mesh, in_specs=(seq_spec, P(), P()), out_specs=seq_spec, check_vma=False)
```
